32 devices in a mesh: rows: 8 (over z, x), cols: 4 (over y, core).
Axes of the slice: x: 2, y: 2, z: 4, core: 2. Of those that a mesh axis runs over, the one named last changes fastest.
Arguments:
- source: float32 [1024, 32768], P('rows', 'cols'), may hold values from -6 to 6
- low_row: int32 [1024], replicated, may hold values from 0 to 1022, as said below
- weight_low: float32 [1024], replicated, may hold values from 0 to 1
Outputs:
- mercator: float32 [1024, 32768], P('rows', 'cols')
- level1: float32 [512, 16384], P('rows', 'cols')
- level2: float32 [256, 8192], P('rows', 'cols')
- level3: float32 [128, 4096], P(('rows', 'cols'))
- level4: float32 [64, 2048], P(('rows', 'cols'))
The draws below stay inside these ranges and needn't reach their ends.
Inputs may be any that keep to these rules, and one draw needn't show every extreme that they name: With t = 68 degrees in radians, E = ln tan(pi/4 + t/2), y = E * (1 - (2m + 1) / 2048) and lat = 2 atan(exp(y)) - pi/2, the base row of Mercator row m is floor((t - lat) / t * 1024 - 0.5) clipped to the range; low_row[m] differs from it by at most 2 and is then clipped to the range.
All inputs are finite; a program needn't handle non-finite values.
Results may differ from the reference program's by a relative error of at most 0.00007.
Values sent between devices are 32-bit elements; how exact they have to be, the bound alone decides.
A program may use at most 128 MiB of HBM per device.

```python
import math
import jax
import jax.numpy as jnp

TOTAL = 1024
COLS = 32768


def draw_low_row(key, part):
    window_top = 68.0 * math.pi / 180.0
    north_edge = math.log(math.tan(math.pi / 4 + window_top / 2))
    centres = (2.0 * jnp.arange(TOTAL, dtype=jnp.float32) + 1.0) / (2.0 * TOTAL)
    merc_y = north_edge * (1.0 - centres)
    latitude = 2.0 * jnp.arctan(jnp.exp(merc_y)) - math.pi / 2
    position = (window_top - latitude) / window_top * TOTAL - 0.5
    base_rows = jnp.clip(jnp.floor(position), 0, TOTAL - 2).astype(jnp.int32)
    jitter = jax.random.randint(key, (TOTAL,), -2, 3, dtype=jnp.int32)
    return jnp.clip(base_rows + jitter, 0, TOTAL - 2).astype(jnp.int32)


def shard_levels(rng, extent, shards, low, high):
    def one(axis_at, shards_of):
        draws = jax.random.uniform(jax.random.fold_in(jax.random.fold_in(rng, 6), axis_at), (shards_of,), jnp.float32, low / len(shards), high / len(shards))
        return jnp.repeat(jnp.exp(draws), extent[axis_at] // shards_of).reshape((-1,) + (1,) * (len(extent) - axis_at - 1))

    loudness = one(*shards[0])
    for cut in shards[1:]:
        loudness = loudness * one(*cut)
    return loudness


def normal_values(key, dims, width, reach, split=(), kind=jnp.bfloat16):
    entries = width * jax.random.normal(key, dims, jnp.float32)
    if split:
        entries = entries * shard_levels(key, dims, split, -0.22, 0.18)
    return jnp.clip(entries, -reach, reach).astype(kind)


def setup_inputs(seed: int = 0) -> dict:
    arg_keys = jax.random.split(jax.random.key(seed), 4)
    return {
        "source": normal_values(arg_keys[0], (TOTAL, COLS), 1.0, 6.0, ((0, 8), (1, 4)), jnp.float32),
        "low_row": draw_low_row(jax.random.fold_in(arg_keys[3], 71), 0),
        "weight_low": jnp.clip(jax.random.uniform(arg_keys[2], (TOTAL,), jnp.float32, 0.0, 1.0), 0.0, 1.0),
    }


def blend(columns, low_row, weight_low):
    upper_rows = jnp.take(columns, low_row, axis=0)
    lower_rows = jnp.take(columns, low_row + 1, axis=0)
    scales = weight_low.reshape((-1,) + (1,) * (columns.ndim - 1))
    return scales * upper_rows + (1.0 - scales) * lower_rows


def halve(picture):
    return (picture[0::2, 0::2] + picture[1::2, 0::2] + picture[0::2, 1::2] + picture[1::2, 1::2]) * 0.25


def reference(source, low_row, weight_low):
    mercator = blend(source, low_row, weight_low)
    level1 = halve(mercator)
    level2 = halve(level1)
    level3 = halve(level2)
    level4 = halve(level3)
    return (mercator, level1, level2, level3, level4)
```

```python
import functools
import math

import jax
import jax.numpy as jnp
import numpy as np
from jax import lax
from jax.experimental import pallas as pl
from jax.experimental.pallas import tpu as pltpu
from jax.sharding import PartitionSpec as P

CHUNK = 8
JITTER = 2
MESH = pl.DeviceIdType.MESH


def windows(total, parts):
    top = 68.0 * math.pi / 180.0
    edge = math.log(math.tan(math.pi / 4 + top / 2))
    m = np.arange(total, dtype=np.float64)
    y = edge * (1.0 - (2.0 * m + 1.0) / (2.0 * total))
    lat = 2.0 * np.arctan(np.exp(y)) - math.pi / 2
    pos = (top - lat) / top * total - 0.5
    slack = 0.01 * total / 1024
    first = np.clip(np.floor(pos - slack) - JITTER, 0, total - 2).astype(int)
    last = np.clip(np.floor(pos + slack) + JITTER, 0, total - 2).astype(int) + 1
    block = total // parts
    out = []
    for r in range(parts):
        low = int(first[r * block : (r + 1) * block].min())
        high = int(last[r * block : (r + 1) * block].max()) + 1
        low = low // CHUNK * CHUNK
        high = -(-high // CHUNK) * CHUNK
        assert high <= (r + 1) * block
        out.append((low, high))
    return out


def flows(total, parts):
    block = total // parts
    found = {}
    for d, (low, high) in enumerate(windows(total, parts)):
        for s in range(low // block, d):
            a, b = max(low, s * block), min(high, (s + 1) * block)
            if b > a:
                found[s, d] = ((a - s * block) // CHUNK, (b - a) // CHUNK)
    return found


def table(index, values):
    out = jnp.int32(values[0])
    for i in range(1, len(values)):
        if values[i] != values[i - 1]:
            out = jnp.where(index >= i, jnp.int32(values[i]), out)
    return out


def exchange_kernel(total, parts, source_ref, recv_ref, send_sem, recv_sem):
    me = lax.axis_index("rows")
    moves = flows(total, parts)
    wins = windows(total, parts)
    block = total // parts
    barrier = pltpu.get_barrier_semaphore()

    @pl.loop(1, parts)
    def _(i):
        pl.semaphore_signal(
            barrier, inc=1, device_id={"rows": lax.rem(me + i, parts)}, device_id_type=MESH
        )

    pl.semaphore_wait(barrier, parts - 1)

    def copy(chunk, slot, at, target):
        return pltpu.make_async_remote_copy(
            src_ref=source_ref.at[pl.ds(pl.multiple_of(chunk * CHUNK, CHUNK), CHUNK)],
            dst_ref=recv_ref.at[pl.ds(pl.multiple_of(slot * CHUNK, CHUNK), CHUNK)],
            send_sem=send_sem.at[at],
            recv_sem=recv_sem.at[slot],
            device_id={"rows": target},
            device_id_type=MESH,
        )

    deltas = sorted({d - s for s, d in moves})
    base = jnp.int32(0)
    for delta in deltas:
        first = table(me, [moves.get((s, s + delta), (0, 0))[0] for s in range(parts)])
        count = table(me, [moves.get((s, s + delta), (0, 0))[1] for s in range(parts)])
        slot0 = table(
            me,
            [
                s * (block // CHUNK) + moves[s, s + delta][0] - wins[s + delta][0] // CHUNK
                if (s, s + delta) in moves
                else 0
                for s in range(parts)
            ],
        )
        start = base
        target = lax.rem(me + delta, parts)

        @pl.loop(0, count)
        def _(i):
            copy(first + i, slot0 + i, start + i, target).start()

        base = base + count

    @pl.loop(0, base)
    def _(i):
        copy(0, 0, i, lax.rem(me + 1, parts)).wait_send()

    got = table(me, received(total, parts))

    @pl.loop(0, got)
    def _(i):
        copy(0, i, 0, lax.rem(me + 1, parts)).wait_recv()


def received(total, parts):
    moves = flows(total, parts)
    return [sum(n for (s, d), (_, n) in moves.items() if d == r) for r in range(parts)]


def exchange(source, total, parts):
    moves = flows(total, parts)
    slots = max(max(received(total, parts)), 2)
    slots += slots % 2
    sends = max(sum(n for (s, d), (_, n) in moves.items() if s == r) for r in range(parts))
    return pl.pallas_call(
        functools.partial(exchange_kernel, total, parts),
        out_shape=jax.ShapeDtypeStruct((slots * CHUNK, source.shape[1]), source.dtype),
        in_specs=[pl.BlockSpec(memory_space=pltpu.HBM)],
        out_specs=pl.BlockSpec(memory_space=pltpu.HBM),
        scratch_shapes=[
            pltpu.SemaphoreType.DMA((max(sends, 1),)),
            pltpu.SemaphoreType.DMA((slots,)),
        ],
        compiler_params=pltpu.CompilerParams(collective_id=0, has_side_effects=True),
        name="halo",
    )(source)


def split(x):
    high = x.astype(jnp.bfloat16)
    low = (x - high.astype(jnp.float32)).astype(jnp.bfloat16)
    return high, low


def pool_columns(x, levels):
    rows, width = x.shape
    slab = 128 << levels
    i = lax.broadcasted_iota(jnp.int32, (slab, 128), 0)
    o = lax.broadcasted_iota(jnp.int32, (slab, 128), 1)
    pairing = jnp.where(i >> levels == o, 0.5**levels, 0.0).astype(jnp.bfloat16)
    pieces = width // slab
    stacked = jnp.concatenate([x[:, k * slab : (k + 1) * slab] for k in range(pieces)], axis=0)
    high, low = split(stacked)
    out = jnp.dot(high, pairing, preferred_element_type=jnp.float32)
    out = out + jnp.dot(low, pairing, preferred_element_type=jnp.float32)
    return jnp.concatenate([out[k * rows : (k + 1) * rows] for k in range(pieces)], axis=1)


def pyramid_kernel(
    block, counts, aux_ref, own_ref, recv_ref, merc_ref, one_ref, two_ref, three_ref, wide
):
    slots = recv_ref.shape[0]
    depth = block + slots
    got = table(lax.axis_index("rows"), counts) * CHUNK

    @pl.when(pl.program_id(0) == 0)
    def _():
        col = lax.broadcasted_iota(jnp.int32, (block, depth), 1).astype(jnp.float32)
        weight = aux_ref[:, 2:3]
        band = jnp.where(col == aux_ref[:, 0:1], weight, 0.0)
        band = band + jnp.where(col == aux_ref[:, 1:2], 1.0 - weight, 0.0)
        parts = [band]
        for level in (1, 2, 3):
            o = lax.broadcasted_iota(jnp.int32, (block >> level, block), 0)
            i = lax.broadcasted_iota(jnp.int32, (block >> level, block), 1)
            pool = jnp.where(i >> level == o, 0.5**level, 0.0).astype(jnp.float32)
            parts.append(
                jnp.dot(
                    pool,
                    band,
                    precision=lax.Precision.HIGHEST,
                    preferred_element_type=jnp.float32,
                )
            )
        high, low = split(jnp.concatenate(parts, axis=0))
        wide[0] = high
        wide[1] = low

    row = lax.broadcasted_iota(jnp.int32, recv_ref.shape, 0)
    x = jnp.concatenate([own_ref[...], jnp.where(row < got, recv_ref[...], 0.0)], axis=0)
    high, low = split(x)
    y = jnp.dot(wide[0], high, preferred_element_type=jnp.float32)
    y = y + jnp.dot(wide[0], low, preferred_element_type=jnp.float32)
    y = y + jnp.dot(wide[1], high, preferred_element_type=jnp.float32)
    merc_ref[...] = y[:block]
    at = block
    for level, ref in ((1, one_ref), (2, two_ref), (3, three_ref)):
        n = block >> level
        ref[...] = pool_columns(y[at : at + n], level)
        at += n


def pyramid(aux, source, recv, total, parts):
    block, width = source.shape
    step = math.gcd(width, 1024)
    slots = recv.shape[0]
    wide_rows = block + block // 2 + block // 4 + block // 8
    return pl.pallas_call(
        functools.partial(pyramid_kernel, block, received(total, parts)),
        grid=(width // step,),
        out_shape=[
            jax.ShapeDtypeStruct((block >> k, width >> k), jnp.float32) for k in range(4)
        ],
        in_specs=[
            pl.BlockSpec(aux.shape, lambda j: (0, 0)),
            pl.BlockSpec((block, step), lambda j: (0, j)),
            pl.BlockSpec((slots, step), lambda j: (0, j)),
        ],
        out_specs=[pl.BlockSpec((block >> k, step >> k), lambda j: (0, j)) for k in range(4)],
        scratch_shapes=[pltpu.VMEM((2, wide_rows, block + slots), jnp.bfloat16)],
        name="pyramid",
    )(aux, source, recv)


def halve(x):
    r, c = x.shape
    x = x.reshape(r // 2, 2, c).sum(axis=1)
    i = lax.broadcasted_iota(jnp.int32, (c, c // 2), 0)
    o = lax.broadcasted_iota(jnp.int32, (c, c // 2), 1)
    pairing = jnp.where(i // 2 == o, 0.25, 0.0).astype(jnp.float32)
    return jnp.dot(x, pairing, precision=lax.Precision.HIGHEST)


def body(parts, source, low_row, weight_low):
    total = low_row.shape[0]
    block = source.shape[0]
    me = lax.axis_index("rows")
    recv = exchange(source, total, parts)
    lows = jnp.asarray([w[0] for w in windows(total, parts)], jnp.int32)
    mine = lax.dynamic_slice(low_row, (me * block,), (block,))
    weight = lax.dynamic_slice(weight_low, (me * block,), (block,))

    def place(g):
        return jnp.where(g >= me * block, g - me * block, block + g - lows[me])

    aux = jnp.stack(
        [place(mine).astype(jnp.float32), place(mine + 1).astype(jnp.float32), weight], axis=1
    )
    mercator, level1, level2, level3 = pyramid(aux, source, recv, total, parts)
    level4 = halve(level3)
    level3 = lax.all_to_all(level3, "cols", split_axis=0, concat_axis=1, tiled=True)
    level4 = lax.all_to_all(level4, "cols", split_axis=0, concat_axis=1, tiled=True)
    return mercator, level1, level2, level3, level4


def solution(mesh):
    return jax.shard_map(
        functools.partial(body, mesh.shape["rows"]),
        mesh=mesh,
        in_specs=(P("rows", "cols"), P(), P()),
        out_specs=(
            P("rows", "cols"),
            P("rows", "cols"),
            P("rows", "cols"),
            P(("rows", "cols"), None),
            P(("rows", "cols"), None),
        ),
        check_vma=False,
    )
```

```python
import functools
import math

import jax
import jax.numpy as jnp
import numpy as np
from jax import lax
from jax.experimental import pallas as pl
from jax.experimental.pallas import tpu as pltpu
from jax.sharding import PartitionSpec as P

CHUNK = 8
JITTER = 2
MESH = pl.DeviceIdType.MESH


def windows(total, parts):
    top = 68.0 * math.pi / 180.0
    edge = math.log(math.tan(math.pi / 4 + top / 2))
    m = np.arange(total, dtype=np.float64)
    y = edge * (1.0 - (2.0 * m + 1.0) / (2.0 * total))
    lat = 2.0 * np.arctan(np.exp(y)) - math.pi / 2
    pos = (top - lat) / top * total - 0.5
    slack = 0.01 * total / 1024
    first = np.clip(np.floor(pos - slack) - JITTER, 0, total - 2).astype(int)
    last = np.clip(np.floor(pos + slack) + JITTER, 0, total - 2).astype(int) + 1
    block = total // parts
    out = []
    for r in range(parts):
        low = int(first[r * block : (r + 1) * block].min())
        high = int(last[r * block : (r + 1) * block].max()) + 1
        low = low // CHUNK * CHUNK
        high = -(-high // CHUNK) * CHUNK
        assert high <= (r + 1) * block
        out.append((low, high))
    return out


def flows(total, parts):
    block = total // parts
    found = {}
    for d, (low, high) in enumerate(windows(total, parts)):
        for s in range(low // block, d):
            a, b = max(low, s * block), min(high, (s + 1) * block)
            if b > a:
                found[s, d] = ((a - s * block) // CHUNK, (b - a) // CHUNK)
    return found


def table(index, values):
    out = jnp.int32(values[0])
    for i in range(1, len(values)):
        if values[i] != values[i - 1]:
            out = jnp.where(index >= i, jnp.int32(values[i]), out)
    return out


def relays(total, parts):
    moves = flows(total, parts)
    if max((d - s for s, d in moves), default=0) > 2:
        return {}
    load = {(p, z): 0 for p in (0, 1) for z in range(parts // 2)}
    for (s, d), (_, n) in moves.items():
        if d == s + 1:
            load[s % 2, d // 2] += n
    plan = {}
    while True:
        best = None
        for (s, d), (_, n) in moves.items():
            if d != s + 1:
                continue
            here = d // 2
            for there in (here - 1, here + 1) if s % 2 == 0 else (here - 1,):
                if not 0 <= there < parts // 2:
                    continue
                relay = d + 2 * (there - here)
                used = plan.get((s, d), (relay, 0))
                taken = any(v[0] == relay and k != (s, d) for k, v in plan.items())
                if used[0] != relay or used[1] >= n or taken:
                    continue
                gap = load[s % 2, here] - load[s % 2, there]
                if gap >= 2 and (best is None or gap > best[0]):
                    best = (gap, s, d, here, there, relay, used[1] + 1)
        if best is None:
            return plan
        _, s, d, here, there, relay, n = best
        plan[s, d] = (relay, n)
        load[s % 2, here] -= 1
        load[s % 2, there] += 1


def exchange_kernel(total, parts, source_ref, recv_ref, held, send_sem, recv_sem, held_sem):
    me = lax.axis_index("rows")
    moves = flows(total, parts)
    wins = windows(total, parts)
    plan = relays(total, parts)
    block = total // parts
    barrier = pltpu.get_barrier_semaphore()

    @pl.loop(1, parts)
    def _(i):
        pl.semaphore_signal(
            barrier, inc=1, device_id={"rows": lax.rem(me + i, parts)}, device_id_type=MESH
        )

    pl.semaphore_wait(barrier, parts - 1)

    def chunk_of(ref, at):
        return ref.at[pl.ds(pl.multiple_of(at * CHUNK, CHUNK), CHUNK)]

    def copy(src, dst, at, landed, target):
        return pltpu.make_async_remote_copy(
            src_ref=src,
            dst_ref=dst,
            send_sem=send_sem.at[at],
            recv_sem=landed,
            device_id={"rows": target},
            device_id_type=MESH,
        )

    def slot_of(s, d):
        return s * (block // CHUNK) + moves[s, d][0] - wins[d][0] // CHUNK

    base = jnp.int32(0)
    by_source = {s: (r - s, moves[s, d][0], n) for (s, d), (r, n) in plan.items()}
    for shift in sorted({v[0] for v in by_source.values()}):
        mine = [by_source.get(s, (0, 0, 0)) for s in range(parts)]
        mine = [v if v[0] == shift else (0, 0, 0) for v in mine]
        first = table(me, [v[1] for v in mine])
        count = table(me, [v[2] for v in mine])
        start = base
        target = lax.rem(me + shift + parts, parts)

        @pl.loop(0, count)
        def _(i):
            copy(
                chunk_of(source_ref, first + i),
                chunk_of(held, i),
                start + i,
                held_sem.at[i],
                target,
            ).start()

        base = base + count

    for delta in sorted({d - s for s, d in moves}):
        ours = [(s, s + delta) for s in range(parts)]
        skip = [plan.get(k, (0, 0))[1] for k in ours]
        first = table(me, [moves[k][0] + n if k in moves else 0 for k, n in zip(ours, skip)])
        count = table(me, [moves[k][1] - n if k in moves else 0 for k, n in zip(ours, skip)])
        slot0 = table(me, [slot_of(*k) + n if k in moves else 0 for k, n in zip(ours, skip)])
        start = base
        target = lax.rem(me + delta, parts)

        @pl.loop(0, count)
        def _(i):
            copy(
                chunk_of(source_ref, first + i),
                chunk_of(recv_ref, slot0 + i),
                start + i,
                recv_sem.at[slot0 + i],
                target,
            ).start()

        base = base + count

    by_relay = {r: (d - r, slot_of(s, d), n) for (s, d), (r, n) in plan.items()}
    for shift in sorted({v[0] for v in by_relay.values()}):
        mine = [by_relay.get(r, (0, 0, 0)) for r in range(parts)]
        mine = [v if v[0] == shift else (0, 0, 0) for v in mine]
        slot0 = table(me, [v[1] for v in mine])
        count = table(me, [v[2] for v in mine])
        start = base
        target = lax.rem(me + shift + parts, parts)

        @pl.loop(0, count)
        def _(i):
            forward = copy(
                chunk_of(held, i),
                chunk_of(recv_ref, slot0 + i),
                start + i,
                recv_sem.at[slot0 + i],
                target,
            )
            copy(
                chunk_of(source_ref, 0), chunk_of(held, i), 0, held_sem.at[i], target
            ).wait_recv()
            forward.start()

        base = base + count

    other = lax.rem(me + 1, parts)

    @pl.loop(0, base)
    def _(i):
        copy(
            chunk_of(source_ref, 0), chunk_of(recv_ref, 0), i, recv_sem.at[0], other
        ).wait_send()

    got = table(me, received(total, parts))

    @pl.loop(0, got)
    def _(i):
        copy(
            chunk_of(source_ref, 0), chunk_of(recv_ref, i), 0, recv_sem.at[i], other
        ).wait_recv()


def received(total, parts):
    moves = flows(total, parts)
    return [sum(n for (s, d), (_, n) in moves.items() if d == r) for r in range(parts)]


def exchange(source, total, parts):
    moves = flows(total, parts)
    slots = max(max(received(total, parts)), 2)
    slots += slots % 2
    plan = relays(total, parts)
    sends = max(
        sum(n for (s, d), (_, n) in moves.items() if s == p)
        + sum(n for r, n in plan.values() if r == p)
        for p in range(parts)
    )
    hold = max([n for _, n in plan.values()], default=1)
    return pl.pallas_call(
        functools.partial(exchange_kernel, total, parts),
        out_shape=jax.ShapeDtypeStruct((slots * CHUNK, source.shape[1]), source.dtype),
        in_specs=[pl.BlockSpec(memory_space=pltpu.HBM)],
        out_specs=pl.BlockSpec(memory_space=pltpu.HBM),
        scratch_shapes=[
            pltpu.VMEM((hold * CHUNK, source.shape[1]), source.dtype),
            pltpu.SemaphoreType.DMA((max(sends, 1),)),
            pltpu.SemaphoreType.DMA((slots,)),
            pltpu.SemaphoreType.DMA((hold,)),
        ],
        compiler_params=pltpu.CompilerParams(collective_id=0, has_side_effects=True),
        name="halo",
    )(source)


def split(x):
    high = x.astype(jnp.bfloat16)
    low = (x - high.astype(jnp.float32)).astype(jnp.bfloat16)
    return high, low


def pool_columns(x, levels):
    rows, width = x.shape
    slab = 128 << levels
    i = lax.broadcasted_iota(jnp.int32, (slab, 128), 0)
    o = lax.broadcasted_iota(jnp.int32, (slab, 128), 1)
    pairing = jnp.where(i >> levels == o, 0.5**levels, 0.0).astype(jnp.bfloat16)
    pieces = width // slab
    stacked = jnp.concatenate([x[:, k * slab : (k + 1) * slab] for k in range(pieces)], axis=0)
    high, low = split(stacked)
    out = jnp.dot(high, pairing, preferred_element_type=jnp.float32)
    out = out + jnp.dot(low, pairing, preferred_element_type=jnp.float32)
    return jnp.concatenate([out[k * rows : (k + 1) * rows] for k in range(pieces)], axis=1)


def pyramid_kernel(
    total, parts, low_ref, weight_ref, own_ref, recv_ref, merc_ref, one_ref, two_ref, three_ref, wide
):
    block = own_ref.shape[0]
    slots = recv_ref.shape[0]
    depth = block + slots
    me = lax.axis_index("rows")
    got = table(me, received(total, parts)) * CHUNK

    @pl.when(pl.program_id(0) == 0)
    def _():
        begin = table(me, [w[0] for w in windows(total, parts)])
        low = low_ref[pl.ds(me, 1), :]
        weight = weight_ref[pl.ds(me, 1), :]

        def place(g):
            return jnp.where(g >= me * block, g - me * block, block + g - begin)

        k = lax.broadcasted_iota(jnp.int32, (depth, block), 0)
        band = jnp.where(k == place(low), weight, 0.0)
        band = band + jnp.where(k == place(low + 1), 1.0 - weight, 0.0)
        pools = []
        for level in range(4):
            o = lax.broadcasted_iota(jnp.int32, (block >> level, block), 0)
            i = lax.broadcasted_iota(jnp.int32, (block >> level, block), 1)
            pools.append(jnp.where(i >> level == o, 0.5**level, 0.0).astype(jnp.float32))
        rows = lax.dot_general(
            jnp.concatenate(pools, axis=0),
            band,
            (((1,), (1,)), ((), ())),
            precision=lax.Precision.HIGHEST,
            preferred_element_type=jnp.float32,
        )
        high, low_part = split(rows)
        wide[...] = jnp.concatenate([high, high, low_part], axis=1)

    row = lax.broadcasted_iota(jnp.int32, recv_ref.shape, 0)
    x = jnp.concatenate([own_ref[...], jnp.where(row < got, recv_ref[...], 0.0)], axis=0)
    high, low_part = split(x)
    stacked = jnp.concatenate([high, low_part, high], axis=0)
    y = jnp.dot(wide[...], stacked, preferred_element_type=jnp.float32)
    merc_ref[...] = y[:block]
    at = block
    for level, ref in ((1, one_ref), (2, two_ref)):
        n = block >> level
        ref[...] = pool_columns(y[at : at + n], level)
        at += n
    three = pool_columns(y[at:], 3)
    each = three_ref.shape[1]
    for i in range(three_ref.shape[0]):
        three_ref[i] = three[i * each : (i + 1) * each]


def pyramid(low_row, weight_low, source, recv, total, parts, owners):
    block, width = source.shape
    step = math.gcd(width, 1024)
    slots = recv.shape[0]
    wide_rows = block + block // 2 + block // 4 + block // 8
    each = (block >> 3) // owners
    return pl.pallas_call(
        functools.partial(pyramid_kernel, total, parts),
        grid=(width // step,),
        out_shape=[jax.ShapeDtypeStruct((block >> k, width >> k), jnp.float32) for k in range(3)]
        + [jax.ShapeDtypeStruct((owners, each, width >> 3), jnp.float32)],
        in_specs=[
            pl.BlockSpec((parts, block), lambda j: (0, 0)),
            pl.BlockSpec((parts, block), lambda j: (0, 0)),
            pl.BlockSpec((block, step), lambda j: (0, j)),
            pl.BlockSpec((slots, step), lambda j: (0, j)),
        ],
        out_specs=[pl.BlockSpec((block >> k, step >> k), lambda j: (0, j)) for k in range(3)]
        + [pl.BlockSpec((owners, each, step >> 3), lambda j: (0, 0, j))],
        scratch_shapes=[pltpu.VMEM((wide_rows, 3 * (block + slots)), jnp.bfloat16)],
        name="pyramid",
    )(low_row.reshape(parts, block), weight_low.reshape(parts, block), source, recv)


def share_kernel(owners, three_ref, rows_ref, pooled_ref, landed, send_sem, recv_sem):
    me = lax.axis_index("cols")
    width = three_ref.shape[2]
    barrier = pltpu.get_barrier_semaphore()
    for i in range(1, owners):
        pl.semaphore_signal(
            barrier, inc=1, device_id={"cols": lax.rem(me + i, owners)}, device_id_type=MESH
        )
    pl.semaphore_wait(barrier, owners - 1)
    copies = []
    for i in range(1, owners):
        target = lax.rem(me + i, owners)
        copies.append(
            pltpu.make_async_remote_copy(
                src_ref=three_ref.at[target],
                dst_ref=landed.at[owners - i],
                send_sem=send_sem.at[i],
                recv_sem=recv_sem.at[owners - i],
                device_id={"cols": target},
                device_id_type=MESH,
            )
        )
    for c in copies:
        c.start()
    levels = 1
    slab = 128 << levels
    i = lax.broadcasted_iota(jnp.int32, (slab, 128), 0)
    o = lax.broadcasted_iota(jnp.int32, (slab, 128), 1)
    pairing = jnp.where(i >> levels == o, 0.25, 0.0).astype(jnp.bfloat16)

    def place(piece, column):
        rows_ref[:, pl.ds(pl.multiple_of(column * width, 128), width)] = piece
        pairs = piece.shape[0] // 2
        sums = jnp.concatenate(
            [piece[2 * p : 2 * p + 1] + piece[2 * p + 1 : 2 * p + 2] for p in range(pairs)], axis=0
        )
        flat = jnp.concatenate(
            [sums[:, k * slab : (k + 1) * slab] for k in range(width // slab)], axis=0
        )
        high, low_part = split(flat)
        out = jnp.dot(high, pairing, preferred_element_type=jnp.float32)
        out = out + jnp.dot(low_part, pairing, preferred_element_type=jnp.float32)
        out = jnp.concatenate(
            [out[k * pairs : (k + 1) * pairs] for k in range(width // slab)], axis=1
        )
        half = width // 2
        pooled_ref[:, pl.ds(pl.multiple_of(column * half, 128), half)] = out

    place(three_ref[me], me)
    for i in range(1, owners):
        copies[owners - i - 1].wait_recv()
        place(landed[i], lax.rem(me + i, owners))
    for c in copies:
        c.wait_send()


def share(three):
    owners, each, width = three.shape
    return pl.pallas_call(
        functools.partial(share_kernel, owners),
        out_shape=[
            jax.ShapeDtypeStruct((each, owners * width), jnp.float32),
            jax.ShapeDtypeStruct((each // 2, owners * width // 2), jnp.float32),
        ],
        in_specs=[pl.BlockSpec(memory_space=pltpu.VMEM)],
        out_specs=[pl.BlockSpec(memory_space=pltpu.VMEM)] * 2,
        scratch_shapes=[
            pltpu.VMEM(three.shape, jnp.float32),
            pltpu.SemaphoreType.DMA((owners,)),
            pltpu.SemaphoreType.DMA((owners,)),
        ],
        compiler_params=pltpu.CompilerParams(collective_id=1, has_side_effects=True),
        name="share",
    )(three)


def body(parts, owners, source, low_row, weight_low):
    total = low_row.shape[0]
    recv = exchange(source, total, parts)
    mercator, level1, level2, three = pyramid(
        low_row, weight_low, source, recv, total, parts, owners
    )
    level3, level4 = share(three)
    return mercator, level1, level2, level3, level4


def solution(mesh):
    return jax.shard_map(
        functools.partial(body, mesh.shape["rows"], mesh.shape["cols"]),
        mesh=mesh,
        in_specs=(P("rows", "cols"), P(), P()),
        out_specs=(
            P("rows", "cols"),
            P("rows", "cols"),
            P("rows", "cols"),
            P(("rows", "cols"), None),
            P(("rows", "cols"), None),
        ),
        check_vma=False,
    )
```

```python
import functools
import math

import jax
import jax.numpy as jnp
import numpy as np
from jax import lax
from jax.experimental import pallas as pl
from jax.experimental.pallas import tpu as pltpu
from jax.sharding import PartitionSpec as P

CHUNK = 8
SPLIT = 2
STEP = 2048
JITTER = 2
MESH = pl.DeviceIdType.MESH


def windows(total, parts):
    top = 68.0 * math.pi / 180.0
    edge = math.log(math.tan(math.pi / 4 + top / 2))
    m = np.arange(total, dtype=np.float64)
    y = edge * (1.0 - (2.0 * m + 1.0) / (2.0 * total))
    lat = 2.0 * np.arctan(np.exp(y)) - math.pi / 2
    pos = (top - lat) / top * total - 0.5
    slack = 0.01 * total / 1024
    first = np.clip(np.floor(pos - slack) - JITTER, 0, total - 2).astype(int)
    last = np.clip(np.floor(pos + slack) + JITTER, 0, total - 2).astype(int) + 1
    block = total // parts
    out = []
    for r in range(parts):
        low = int(first[r * block : (r + 1) * block].min())
        high = int(last[r * block : (r + 1) * block].max()) + 1
        low = low // CHUNK * CHUNK
        high = -(-high // CHUNK) * CHUNK
        assert high <= (r + 1) * block
        out.append((low, high))
    return out


def flows(total, parts):
    block = total // parts
    found = {}
    for d, (low, high) in enumerate(windows(total, parts)):
        for s in range(low // block, d):
            a, b = max(low, s * block), min(high, (s + 1) * block)
            if b > a:
                found[s, d] = ((a - s * block) // CHUNK, (b - a) // CHUNK)
    return found


def units(total, parts):
    return {k: (a * SPLIT, n * SPLIT) for k, (a, n) in flows(total, parts).items()}


def table(index, values):
    out = jnp.int32(values[0])
    for i in range(1, len(values)):
        if values[i] != values[i - 1]:
            out = jnp.where(index >= i, jnp.int32(values[i]), out)
    return out


def relays(total, parts):
    moves = units(total, parts)
    pairs = parts // 2
    if max((d - s for s, d in moves), default=0) > 2 or parts % 2:
        return {}
    plan, taken, before = {}, set(), {}
    for parity in (0, 1):
        flow = [(2 * z - parity, 2 * z - parity + 1) for z in range(pairs)]
        load = [moves.get(k, (0, 0))[1] for k in flow]
        goal = [sum(load) // pairs + (z < sum(load) % pairs) for z in range(pairs)]
        across = 0
        for z in range(pairs - 1):
            across += load[z] - goal[z]
            key = flow[z] if across > 0 else flow[z + 1]
            relay = key[1] + (2 if across > 0 else -2)
            used = before.get(key, 0)
            n = min(abs(across), moves.get(key, (0, 0))[1] - used)
            if n <= 0 or relay in taken or relay == key[0] or (parity and across > 0):
                continue
            plan[key + (relay,)] = (used, n)
            before[key] = used + n
            taken.add(relay)
    return plan


def exchange_kernel(total, parts, source_ref, recv_ref, held, send_sem, recv_sem, held_sem):
    me = lax.axis_index("rows")
    moves = units(total, parts)
    wins = windows(total, parts)
    plan = relays(total, parts)
    block = total // parts
    barrier = pltpu.get_barrier_semaphore()

    @pl.loop(1, parts)
    def _(i):
        pl.semaphore_signal(
            barrier, inc=1, device_id={"rows": lax.rem(me + i, parts)}, device_id_type=MESH
        )

    pl.semaphore_wait(barrier, parts - 1)

    piece = source_ref.shape[1] // SPLIT

    def chunk_of(ref, at):
        rows = pl.ds(pl.multiple_of(lax.div(at, SPLIT) * CHUNK, CHUNK), CHUNK)
        columns = pl.ds(pl.multiple_of(lax.rem(at, SPLIT) * piece, piece), piece)
        return ref.at[rows, columns]

    def held_at(i):
        return held.at[pl.ds(pl.multiple_of(i * CHUNK, CHUNK), CHUNK)]

    def copy(src, dst, at, landed, target):
        return pltpu.make_async_remote_copy(
            src_ref=src,
            dst_ref=dst,
            send_sem=send_sem.at[at],
            recv_sem=landed,
            device_id={"rows": target},
            device_id_type=MESH,
        )

    def slot_of(s, d):
        return (s * block - wins[d][0]) // CHUNK * SPLIT + moves[s, d][0]

    base = jnp.int32(0)
    by_source = {(s, r - s): (moves[s, d][0] + a, n) for (s, d, r), (a, n) in plan.items()}
    for shift in sorted({k[1] for k in by_source}):
        mine = [by_source.get((s, shift), (0, 0)) for s in range(parts)]
        first = table(me, [v[0] for v in mine])
        count = table(me, [v[1] for v in mine])
        start = base
        target = lax.rem(me + shift + parts, parts)

        @pl.loop(0, count)
        def _(i):
            copy(
                chunk_of(source_ref, first + i),
                held_at(i),
                start + i,
                held_sem.at[i],
                target,
            ).start()

        base = base + count

    for delta in sorted({d - s for s, d in moves}):
        ours = [(s, s + delta) for s in range(parts)]
        skip = [sum(v[1] for p, v in plan.items() if p[:2] == k) for k in ours]
        first = table(me, [moves[k][0] + n if k in moves else 0 for k, n in zip(ours, skip)])
        count = table(me, [moves[k][1] - n if k in moves else 0 for k, n in zip(ours, skip)])
        slot0 = table(me, [slot_of(*k) + n if k in moves else 0 for k, n in zip(ours, skip)])
        start = base
        target = lax.rem(me + delta, parts)

        @pl.loop(0, count)
        def _(i):
            copy(
                chunk_of(source_ref, first + i),
                chunk_of(recv_ref, slot0 + i),
                start + i,
                recv_sem.at[slot0 + i],
                target,
            ).start()

        base = base + count

    by_relay = {(r, d - r): (slot_of(s, d) + a, n) for (s, d, r), (a, n) in plan.items()}
    for shift in sorted({k[1] for k in by_relay}):
        mine = [by_relay.get((r, shift), (0, 0)) for r in range(parts)]
        slot0 = table(me, [v[0] for v in mine])
        count = table(me, [v[1] for v in mine])
        start = base
        target = lax.rem(me + shift + parts, parts)

        @pl.loop(0, count)
        def _(i):
            forward = copy(
                held_at(i),
                chunk_of(recv_ref, slot0 + i),
                start + i,
                recv_sem.at[slot0 + i],
                target,
            )
            copy(
                chunk_of(source_ref, jnp.int32(0)), held_at(i), 0, held_sem.at[i], target
            ).wait_recv()
            forward.start()

        base = base + count

    other = lax.rem(me + 1, parts)

    @pl.loop(0, base)
    def _(i):
        copy(
            chunk_of(source_ref, jnp.int32(0)), chunk_of(recv_ref, jnp.int32(0)), i, recv_sem.at[0], other
        ).wait_send()

    got = table(me, received(total, parts)) * SPLIT

    @pl.loop(0, got)
    def _(i):
        copy(
            chunk_of(source_ref, jnp.int32(0)), chunk_of(recv_ref, i), 0, recv_sem.at[i], other
        ).wait_recv()


def received(total, parts):
    moves = flows(total, parts)
    return [sum(n for (s, d), (_, n) in moves.items() if d == r) for r in range(parts)]


def exchange(source, total, parts):
    moves = units(total, parts)
    slots = max(max(received(total, parts)), 2)
    slots += slots % 2
    plan = relays(total, parts)
    sends = max(
        sum(n for (s, d), (_, n) in moves.items() if s == p)
        + sum(n for (_, _, r), (_, n) in plan.items() if r == p)
        for p in range(parts)
    )
    hold = max([n for _, n in plan.values()], default=1)
    return pl.pallas_call(
        functools.partial(exchange_kernel, total, parts),
        out_shape=jax.ShapeDtypeStruct((slots * CHUNK, source.shape[1]), source.dtype),
        in_specs=[pl.BlockSpec(memory_space=pltpu.HBM)],
        out_specs=pl.BlockSpec(memory_space=pltpu.HBM),
        scratch_shapes=[
            pltpu.VMEM((hold * CHUNK, source.shape[1] // SPLIT), source.dtype),
            pltpu.SemaphoreType.DMA((max(sends, 1),)),
            pltpu.SemaphoreType.DMA((slots * SPLIT,)),
            pltpu.SemaphoreType.DMA((hold,)),
        ],
        compiler_params=pltpu.CompilerParams(collective_id=0, has_side_effects=True),
        name="halo",
    )(source)


def split(x):
    high = x.astype(jnp.bfloat16)
    low = (x - high.astype(jnp.float32)).astype(jnp.bfloat16)
    return high, low


def pool_columns(x, levels):
    rows, width = x.shape
    slab = 128 << levels
    i = lax.broadcasted_iota(jnp.int32, (slab, 128), 0)
    o = lax.broadcasted_iota(jnp.int32, (slab, 128), 1)
    pairing = jnp.where(i >> levels == o, 0.5**levels, 0.0).astype(jnp.bfloat16)
    pieces = width // slab
    stacked = jnp.concatenate([x[:, k * slab : (k + 1) * slab] for k in range(pieces)], axis=0)
    high, low = split(stacked)
    out = jnp.dot(high, pairing, preferred_element_type=jnp.float32)
    out = out + jnp.dot(low, pairing, preferred_element_type=jnp.float32)
    return jnp.concatenate([out[k * rows : (k + 1) * rows] for k in range(pieces)], axis=1)


def pyramid_kernel(
    total, parts, low_ref, weight_ref, own_ref, recv_ref, merc_ref, one_ref, two_ref, three_ref, wide
):
    block = own_ref.shape[0]
    slots = recv_ref.shape[0]
    depth = block + slots
    me = lax.axis_index("rows")
    got = table(me, received(total, parts)) * CHUNK

    @pl.when(pl.program_id(0) == 0)
    def _():
        begin = table(me, [w[0] for w in windows(total, parts)])
        low = low_ref[pl.ds(me, 1), :]
        weight = weight_ref[pl.ds(me, 1), :]

        def place(g):
            return jnp.where(g >= me * block, g - me * block, block + g - begin)

        k = lax.broadcasted_iota(jnp.int32, (depth, block), 0)
        band = jnp.where(k == place(low), weight, 0.0)
        band = band + jnp.where(k == place(low + 1), 1.0 - weight, 0.0)
        pools = []
        for level in range(4):
            o = lax.broadcasted_iota(jnp.int32, (block >> level, block), 0)
            i = lax.broadcasted_iota(jnp.int32, (block >> level, block), 1)
            pools.append(jnp.where(i >> level == o, 0.5**level, 0.0).astype(jnp.float32))
        rows = lax.dot_general(
            jnp.concatenate(pools, axis=0),
            band,
            (((1,), (1,)), ((), ())),
            precision=lax.Precision.HIGHEST,
            preferred_element_type=jnp.float32,
        )
        high, low_part = split(rows)
        wide[...] = jnp.concatenate([high, high, low_part], axis=1)

    row = lax.broadcasted_iota(jnp.int32, recv_ref.shape, 0)
    x = jnp.concatenate([own_ref[...], jnp.where(row < got, recv_ref[...], 0.0)], axis=0)
    high, low_part = split(x)
    stacked = jnp.concatenate([high, low_part, high], axis=0)
    y = jnp.dot(wide[...], stacked, preferred_element_type=jnp.float32)
    merc_ref[...] = y[:block]
    at = block
    for level, ref in ((1, one_ref), (2, two_ref)):
        n = block >> level
        ref[...] = pool_columns(y[at : at + n], level)
        at += n
    three = pool_columns(y[at:], 3)
    each = three_ref.shape[1]
    for i in range(three_ref.shape[0]):
        three_ref[i] = three[i * each : (i + 1) * each]


def pyramid(low_row, weight_low, source, recv, total, parts, owners):
    block, width = source.shape
    step = math.gcd(width, STEP)
    slots = recv.shape[0]
    wide_rows = block + block // 2 + block // 4 + block // 8
    each = (block >> 3) // owners
    return pl.pallas_call(
        functools.partial(pyramid_kernel, total, parts),
        grid=(width // step,),
        out_shape=[jax.ShapeDtypeStruct((block >> k, width >> k), jnp.float32) for k in range(3)]
        + [jax.ShapeDtypeStruct((owners, each, width >> 3), jnp.float32)],
        in_specs=[
            pl.BlockSpec((parts, block), lambda j: (0, 0)),
            pl.BlockSpec((parts, block), lambda j: (0, 0)),
            pl.BlockSpec((block, step), lambda j: (0, j)),
            pl.BlockSpec((slots, step), lambda j: (0, j)),
        ],
        out_specs=[pl.BlockSpec((block >> k, step >> k), lambda j: (0, j)) for k in range(3)]
        + [pl.BlockSpec((owners, each, step >> 3), lambda j: (0, 0, j))],
        scratch_shapes=[pltpu.VMEM((wide_rows, 3 * (block + slots)), jnp.bfloat16)],
        name="pyramid",
    )(low_row.reshape(parts, block), weight_low.reshape(parts, block), source, recv)


def share_kernel(owners, three_ref, landed, send_sem, recv_sem, own_sem):
    me = lax.axis_index("cols")
    barrier = pltpu.get_barrier_semaphore()
    for i in range(1, owners):
        pl.semaphore_signal(
            barrier, inc=1, device_id={"cols": lax.rem(me + i, owners)}, device_id_type=MESH
        )
    own = pltpu.make_async_copy(three_ref.at[me], landed.at[0], own_sem)
    own.start()
    pl.semaphore_wait(barrier, owners - 1)
    copies = []
    for i in range(1, owners):
        target = lax.rem(me + i, owners)
        copies.append(
            pltpu.make_async_remote_copy(
                src_ref=three_ref.at[target],
                dst_ref=landed.at[owners - i],
                send_sem=send_sem.at[i],
                recv_sem=recv_sem.at[owners - i],
                device_id={"cols": target},
                device_id_type=MESH,
            )
        )
    for c in copies:
        c.start()
    own.wait()
    for c in copies:
        c.wait()


def finish_kernel(landed, rows_ref, pooled_ref):
    owners, each, width = landed.shape
    me = lax.axis_index("cols")
    pairs = each // 2
    slab = 256
    i = lax.broadcasted_iota(jnp.int32, (slab, 128), 0)
    o = lax.broadcasted_iota(jnp.int32, (slab, 128), 1)
    pairing = jnp.where(i >> 1 == o, 0.25, 0.0).astype(jnp.bfloat16)
    pieces = [landed[lax.rem(c - me + owners, owners)] for c in range(owners)]
    x = jnp.concatenate(pieces, axis=1)
    rows_ref[...] = x
    sums = jnp.concatenate(
        [x[2 * p : 2 * p + 1] + x[2 * p + 1 : 2 * p + 2] for p in range(pairs)], axis=0
    )
    count = owners * width // slab
    flat = jnp.concatenate([sums[:, k * slab : (k + 1) * slab] for k in range(count)], axis=0)
    high, low_part = split(flat)
    out = jnp.dot(high, pairing, preferred_element_type=jnp.float32)
    out = out + jnp.dot(low_part, pairing, preferred_element_type=jnp.float32)
    pooled_ref[...] = jnp.concatenate(
        [out[k * pairs : (k + 1) * pairs] for k in range(count)], axis=1
    )


def share(three):
    owners, each, width = three.shape
    landed = pl.pallas_call(
        functools.partial(share_kernel, owners),
        out_shape=jax.ShapeDtypeStruct(three.shape, jnp.float32),
        in_specs=[pl.BlockSpec(memory_space=pltpu.HBM)],
        out_specs=pl.BlockSpec(memory_space=pltpu.HBM),
        scratch_shapes=[
            pltpu.SemaphoreType.DMA((owners,)),
            pltpu.SemaphoreType.DMA((owners,)),
            pltpu.SemaphoreType.DMA,
        ],
        compiler_params=pltpu.CompilerParams(collective_id=1, has_side_effects=True),
        name="share",
    )(three)
    return pl.pallas_call(
        finish_kernel,
        out_shape=[
            jax.ShapeDtypeStruct((each, owners * width), jnp.float32),
            jax.ShapeDtypeStruct((each // 2, owners * width // 2), jnp.float32),
        ],
        in_specs=[pl.BlockSpec(memory_space=pltpu.VMEM)],
        out_specs=[pl.BlockSpec(memory_space=pltpu.VMEM)] * 2,
        name="finish",
    )(landed)


def body(parts, owners, source, low_row, weight_low):
    total = low_row.shape[0]
    recv = exchange(source, total, parts)
    mercator, level1, level2, three = pyramid(
        low_row, weight_low, source, recv, total, parts, owners
    )
    level3, level4 = share(three)
    return mercator, level1, level2, level3, level4


def solution(mesh):
    return jax.shard_map(
        functools.partial(body, mesh.shape["rows"], mesh.shape["cols"]),
        mesh=mesh,
        in_specs=(P("rows", "cols"), P(), P()),
        out_specs=(
            P("rows", "cols"),
            P("rows", "cols"),
            P("rows", "cols"),
            P(("rows", "cols"), None),
            P(("rows", "cols"), None),
        ),
        check_vma=False,
    )
```
